32 devices in a mesh: freq: 2 (over y), src: 8 (over z, x), rcv: 2 (over core).
Axes of the slice: x: 2, y: 2, z: 4, core: 2. Of those that a mesh axis runs over, the one named last changes fastest.
Arguments:
- panel: float32 [4, 1024, 5632], P('freq', 'src', 'rcv'), parts along dimension 0, may hold values from -6 to 6
- obliquity: float32 [4, 131072], P('freq'), parts along dimension 0, may hold values from -0.125 to 0.125
- panel_stations: int32 [1024], replicated, may hold values from 0 to 131071
- tile_map: int32 [512, 2], P('freq'), parts along dimension 0, may hold values from -1 to 21, as said below
- recorded: float32 [256, 4, 256, 256], P(('src', 'rcv'), 'freq'), parts along dimension 1, may hold values from -6 to 6
Outputs:
- demultiple: float32 [256, 4, 256, 256], P(('src', 'rcv'), 'freq'), parts along dimension 1
The draws below stay inside these ranges and needn't reach their ends.
There are 2 independent parts, one for each index of `freq`. The reference program is written for one: setup_inputs(seed, part) draws one part's arguments, and reference() takes and returns one part's arrays. A program takes and returns all parts, laid end to end along the dimension named above; an argument that names none is the same for every part. Nothing has to cross between parts.
Inputs may be any that keep to these rules, and one draw needn't show every extreme that they name: `tile_map`: each slot holds a row tile i and a column tile j with j <= i; each of the 253 such tiles stands in exactly one slot; remaining slots hold -1 in both entries.
All inputs are finite; a program needn't handle non-finite values.
Results may differ from the reference program's by a relative error of at most 0.0044.
Values may be sent and summed in bfloat16 or wider, within the bound.
A program may use at most 192 MiB of HBM per device.

```python
import jax
import jax.numpy as jnp
import numpy as np
from jax import lax

TB = 256
G = 22
NSTAT = 131072
K = 1024
NW = 5632
DEVS_PART = 16
TILE_DEV = 16
SLOTS = 256


def draw_tile_map(key, part):
    rows_np, cols_np = np.tril_indices(G)
    nlow = G * (G + 1) // 2
    order = jax.random.permutation(key, nlow)
    rank = jnp.arange(nlow, dtype=jnp.int32)
    slot = rank % DEVS_PART * TILE_DEV + rank // DEVS_PART
    pairs = jnp.stack([jnp.asarray(rows_np, dtype=jnp.int32)[order], jnp.asarray(cols_np, dtype=jnp.int32)[order]], axis=1)
    filled = jnp.full((SLOTS, 2), -1, dtype=jnp.int32)
    return filled.at[slot].set(pairs)


def with_ends(result, rng, low, top_value):
    index_at = [jax.random.randint(jax.random.fold_in(rng, axis), (), 0, length) for axis, length in enumerate(result.shape)]
    main_axis = result.shape.index(max(result.shape))
    neighbour = index_at[:main_axis] + [(index_at[main_axis] + 1) % result.shape[main_axis]] + index_at[main_axis + 1:]
    return result.at[tuple(index_at)].set(low).at[tuple(neighbour)].set(top_value)


def level_of(stream_key, dims, pieces, smallest, largest):
    gain = 1.0
    for position, blocks in pieces:
        steps = jax.random.uniform(jax.random.fold_in(jax.random.fold_in(stream_key, 6), position), (blocks,), jnp.float32, smallest / len(pieces), largest / len(pieces))
        gain = gain * jnp.repeat(jnp.exp(steps), dims[position] // blocks).reshape((-1,) + (1,) * (len(dims) - 1 - position))
    return gain


def noise(stream_key, extent, width, limit, cuts=(), held_as=jnp.bfloat16):
    drawn = jax.random.normal(stream_key, extent, jnp.float32) * width
    if len(cuts) > 0:
        drawn = level_of(stream_key, extent, cuts, -0.22, 0.18) * drawn
    return jnp.clip(drawn, min=-limit, max=limit).astype(held_as)


def setup_inputs(seed: int = 0, part: int = 0) -> dict:
    streams_of = jax.random.split(jax.random.key(seed), 6)
    part_splits = jax.random.split(jax.random.fold_in(streams_of[5], part), 6)
    panel = noise(part_splits[0], (2, K, NW), 1.0, 6.0, ((1, 8), (2, 2)), jnp.float32)
    obliquity = noise(part_splits[1], (2, NSTAT), (2 * K) ** -0.5, 0.125, (), jnp.float32)
    panel_stations = with_ends(jax.random.randint(streams_of[2], (K,), 0, NSTAT), jax.random.fold_in(streams_of[2], 1), 0, NSTAT - 1).astype(jnp.int32)
    tile_map = draw_tile_map(jax.random.fold_in(jax.random.fold_in(streams_of[5], part), 71), part)
    recorded = noise(part_splits[4], (SLOTS, 2, TB, TB), 1.0, 6.0, ((0, 16),), jnp.float32)
    return dict(panel=panel, obliquity=obliquity, panel_stations=panel_stations, tile_map=tile_map, recorded=recorded)


def reference(panel, obliquity, panel_stations, tile_map, recorded):
    weight_k = jnp.take(obliquity, panel_stations, axis=1)
    panel_b = panel.astype(jnp.bfloat16).astype(jnp.float32)
    w_real = weight_k[0][:, None]
    w_imag = weight_k[1][:, None]
    weighted = jnp.stack([w_real * panel_b[0] - w_imag * panel_b[1], w_real * panel_b[1] + w_imag * panel_b[0]])
    weighted = weighted.astype(jnp.bfloat16).astype(jnp.float32)
    hp = lax.Precision.HIGHEST

    def one_slot(slot):
        row_tile = tile_map[slot, 0]
        col_tile = tile_map[slot, 1]
        valid = (row_tile >= 0).astype(jnp.float32)
        row_start = (jnp.maximum(row_tile, 0) * TB).astype(jnp.int32)
        col_start = (jnp.maximum(col_tile, 0) * TB).astype(jnp.int32)
        left = lax.dynamic_slice_in_dim(weighted, row_start, TB, 2)
        right = lax.dynamic_slice_in_dim(panel_b, col_start, TB, 2)
        real_part = jnp.dot(left[0].T, right[0], precision=hp) - jnp.dot(left[1].T, right[1], precision=hp)
        imag_part = jnp.dot(left[0].T, right[1], precision=hp) + jnp.dot(left[1].T, right[0], precision=hp)
        return recorded[slot] - valid * jnp.stack([real_part, imag_part])

    return lax.map(one_slot, jnp.arange(SLOTS, dtype=jnp.int32))
```

```python
import functools

import jax
import jax.numpy as jnp
from jax import lax
from jax.experimental import pallas as pl
from jax.experimental.pallas import tpu as pltpu
from jax.sharding import PartitionSpec as P

MESH = pl.DeviceIdType.MESH
pin = pltpu.with_memory_space_constraint
LANES = 128
ROWS = 8


def ring_position(index, n):
    if n % 2:
        return index
    half = index // 2
    odd = index % 2
    return odd * (n - 1 - half) + (1 - odd) * half


def ring_member(position, n):
    if n % 2:
        return position
    upper = position // (n // 2)
    return upper * (2 * (n - 1 - position) + 1) + (1 - upper) * 2 * position


def weighted_tile(weight, row_block, sign):
    spread = row_block.shape[-1] // LANES
    w_real = jnp.concatenate([weight[0] * sign] * spread, axis=1)
    w_imag = jnp.concatenate([weight[1] * sign] * spread, axis=1)
    p_real = row_block[0].astype(jnp.float32)
    p_imag = row_block[1].astype(jnp.float32)
    return [w_real * p_real - w_imag * p_imag, w_real * p_imag + w_imag * p_real]


def stack_rows(blocks):
    if blocks[0].shape[0] % 16:
        blocks = [b.astype(jnp.float32) for b in blocks]
    return jnp.concatenate(blocks, axis=0).astype(jnp.bfloat16)


def tile_product(weights, row_blocks, col_blocks, sign):
    lefts, reals, imags = [], [], []
    for weight, row_block, col_block in zip(weights, row_blocks, col_blocks):
        lefts += weighted_tile(weight, row_block, sign)
        reals += [col_block[0], -col_block[1]]
        imags += [col_block[1], col_block[0]]
    weighted = jnp.concatenate(lefts, axis=0).astype(jnp.bfloat16)
    form = (((0,), (0,)), ((), ()))
    return [
        lax.dot_general(weighted, stack_rows(c), form, preferred_element_type=jnp.float32)
        for c in (reals, imags)
    ]


def slot_tiles(tiles, at):
    row_tile, col_tile = tiles[0, at], tiles[1, at]
    sign = -(jnp.minimum(row_tile, 0) + 1).astype(jnp.float32)
    return jnp.maximum(row_tile, 0), jnp.maximum(col_tile, 0), sign


def pieces(held):
    sizes = [1, 2]
    while sum(sizes) < held - 3:
        sizes.append(min(4, held - 3 - sum(sizes)))
    sizes += [2, 1]
    if sum(sizes) != held:
        sizes = [1] * held
    return [(sum(sizes[:i]), size) for i, size in enumerate(sizes)]


def gather_kernel(n_src, n_rcv, stations_in, tiles_in, panel, lines, recorded, acc, last, weight_out, tiles, *scratch):
    full = n_src // 2 - 1
    own = scratch[0]
    from_left = [own] + list(scratch[1 : 1 + full]) + [last]
    from_right = [own] + list(scratch[1 + full : 1 + 2 * full]) + [last]
    stage, obliquity, weight, stations, ring_send, ring_recv, pair_send, pair_recv, last_sems, first_sems, load_sem, local_sem = scratch[1 + 2 * full :]

    src = lax.axis_index("src")
    rcv = lax.axis_index("rcv")
    kd, side = own.shape[2], own.shape[3]
    slots = acc.shape[0]
    held = own.shape[1] // n_rcv
    cuts = pieces(held)
    mine = pl.ds(rcv * held, held)
    pos = ring_position(src, n_src)
    right = ring_member((pos + 1) % n_src, n_src)
    left = ring_member((pos + n_src - 1) % n_src, n_src)

    def load(part, c):
        at = (part, slice(None), pl.ds(cuts[c][0] * side, cuts[c][1] * side))
        return pltpu.make_async_copy(panel.at[at], stage.at[at], load_sem.at[part, c])

    for part in (0, 1):
        load(part, 0).start()
    barrier = pltpu.get_barrier_semaphore()
    for peer in (left, right):
        pl.semaphore_signal(barrier, inc=1, device_id={"src": peer}, device_id_type=MESH)
    for off in range(1, n_rcv):
        pl.semaphore_signal(barrier, inc=1, device_id={"rcv": (rcv + off) % n_rcv}, device_id_type=MESH)

    for c in range(1, len(cuts)):
        for part in (0, 1):
            load(part, c).start()
    named = pltpu.make_async_copy(stations_in, stations, local_sem.at[2])
    mapped = pltpu.make_async_copy(tiles_in, tiles, local_sem.at[3])
    fetch = pltpu.make_async_copy(lines, obliquity, local_sem.at[0])
    fill = pltpu.make_async_copy(recorded, acc, local_sem.at[1])

    def convert(part, c):
        load(part, c).wait()
        for t in range(cuts[c][0], sum(cuts[c])):
            own[part, rcv * held + t] = stage[part, :, t * side : (t + 1) * side].astype(jnp.bfloat16)

    sides = ((0, from_left, right), (1, from_right, left))

    def ring_copy(d, step, part):
        _, blocks, peer = sides[d]
        return pltpu.make_async_remote_copy(
            src_ref=blocks[step].at[part, mine],
            dst_ref=blocks[step + 1].at[part, mine],
            send_sem=ring_send.at[d, step, part],
            recv_sem=ring_recv.at[d, step, part],
            device_id={"src": peer},
            device_id_type=MESH,
        )

    def pair_copy(d, step, part, off):
        block = sides[d][1][step].at[part, mine]
        return pltpu.make_async_remote_copy(
            src_ref=block,
            dst_ref=block,
            send_sem=pair_send.at[d, step, part, off - 1],
            recv_sem=pair_recv.at[d, step, part, off - 1],
            device_id={"rcv": (rcv + off) % n_rcv},
            device_id_type=MESH,
        )

    def first_ring(d, part, c):
        _, blocks, peer = sides[d]
        at = pl.ds(rcv * held + cuts[c][0], cuts[c][1])
        return pltpu.make_async_remote_copy(
            src_ref=own.at[part, at],
            dst_ref=blocks[1].at[part, at],
            send_sem=first_sems.at[0, d, part, c],
            recv_sem=first_sems.at[1, d, part, c],
            device_id={"src": peer},
            device_id_type=MESH,
        )

    def last_ring(d, c):
        _, blocks, peer = sides[d]
        at = pl.ds(rcv * held + cuts[c][0], cuts[c][1])
        return pltpu.make_async_remote_copy(
            src_ref=blocks[full].at[d, at],
            dst_ref=last.at[d, at],
            send_sem=last_sems.at[0, d, c, 0],
            recv_sem=last_sems.at[1, d, c, 0],
            device_id={"src": peer},
            device_id_type=MESH,
        )

    def last_pair(d, c, off):
        block = last.at[d, pl.ds(rcv * held + cuts[c][0], cuts[c][1])]
        return pltpu.make_async_remote_copy(
            src_ref=block,
            dst_ref=block,
            send_sem=last_sems.at[0, d, c, off],
            recv_sem=last_sems.at[1, d, c, off],
            device_id={"rcv": (rcv + off) % n_rcv},
            device_id_type=MESH,
        )

    def pairs(step, d):
        return d == 0 or step > 0

    def rows_of(owner):
        return pl.ds(pl.multiple_of(owner * kd, kd), kd)

    def product(blocks):
        def one(slot, carry):
            row_tile, col_tile, sign = slot_tiles(tiles, (src * n_rcv + rcv) * slots + slot)
            results = tile_product(
                [(weight[0, rows_of(owner), :], weight[1, rows_of(owner), :]) for _, owner in blocks],
                [jnp.stack([block[0, row_tile], block[1, row_tile]]) for block, _ in blocks],
                [(block[0, col_tile], block[1, col_tile]) for block, _ in blocks],
                sign,
            )
            for part in (0, 1):
                acc[slot, part] += results[part]
            return carry

        lax.fori_loop(0, slots, one, 0)

    def gather_weights():
        lane = lax.broadcasted_iota(jnp.int32, (ROWS, LANES), 1)
        row = lax.broadcasted_iota(jnp.int32, (ROWS, LANES), 0)

        def group(g, carry):
            real = jnp.zeros((ROWS, LANES), jnp.float32)
            imag = jnp.zeros((ROWS, LANES), jnp.float32)
            for u in range(ROWS):
                station = stations[g * ROWS + u]
                line = lax.div(station, LANES)
                pair = obliquity[line]
                hit = (row == u) & (lane == station - line * LANES)
                real = jnp.where(hit, pair[0:1], real)
                imag = jnp.where(hit, pair[1:2], imag)
            at = pl.ds(pl.multiple_of(g * ROWS, ROWS), ROWS)
            weight[0, at, :] = jnp.broadcast_to(jnp.sum(real, axis=1, keepdims=True), (ROWS, LANES))
            weight[1, at, :] = jnp.broadcast_to(jnp.sum(imag, axis=1, keepdims=True), (ROWS, LANES))
            return carry

        lax.fori_loop(0, weight.shape[1] // ROWS, group, 0)

    for c in range(len(cuts)):
        for part in (0, 1):
            convert(part, c)
            if part == 0 and c == 0:
                pl.semaphore_wait(barrier, 1 + n_rcv)
            first_ring(part, part, c).start()
    for d in (0, 1):
        for c in range(len(cuts)):
            first_ring(d, 1 - d, c).start()
    for part in (0, 1):
        for off in range(1, n_rcv):
            pair_copy(0, 0, part, off).start()
    for step in range(full + 1):
        for turn in (0, 1):
            for d in (0, 1):
                part = d if turn == 0 else 1 - d
                if step == 0:
                    continue
                if step == 1:
                    for c in range(len(cuts)):
                        first_ring(d, part, c).wait_recv()
                else:
                    ring_copy(d, step - 1, part).wait_recv()
                if step < full:
                    ring_copy(d, step, part).start()
                elif part == d:
                    for c in range(len(cuts)):
                        last_ring(d, c).start()
                for off in range(1, n_rcv):
                    pair_copy(d, step, part, off).start()
        if step == 0:
            fetch.start()
            named.start()
            mapped.start()
            fill.start()
            fetch.wait()
            named.wait()
            mapped.wait()
            gather_weights()
            fill.wait()
        for part in (0, 1):
            for d in (0, 1):
                if pairs(step, d):
                    for off in range(1, n_rcv):
                        pair_copy(d, step, part, off).wait_recv()
        before = ring_member((pos + n_src - step) % n_src, n_src)
        after = ring_member((pos + step) % n_src, n_src)
        if step == 0:
            blocks = [(own, src)]
        else:
            blocks = [(from_left[step], before), (from_right[step], after)]
        product(blocks)

    opposite = ring_member((pos + n_src // 2) % n_src, n_src)
    weight_out[...] = weight[:, rows_of(opposite), :]
    for step in range(full + 1):
        for part in (0, 1):
            for d in (0, 1):
                if step == 0:
                    for c in range(len(cuts)):
                        first_ring(d, part, c).wait_send()
                elif step < full:
                    ring_copy(d, step, part).wait_send()
                if pairs(step, d):
                    for off in range(1, n_rcv):
                        pair_copy(d, step, part, off).wait_send()
    for c in range(len(cuts)):
        for d in (0, 1):
            last_ring(d, c).wait_recv()
            for off in range(1, n_rcv):
                last_pair(d, c, off).start()
    for c in range(len(cuts)):
        for d in (0, 1):
            for off in range(1, n_rcv):
                last_pair(d, c, off).wait_recv()
    for c in range(len(cuts)):
        for d in (0, 1):
            last_ring(d, c).wait_send()
            for off in range(1, n_rcv):
                last_pair(d, c, off).wait_send()


def finish_kernel(n_rcv, tiles, weight, last, acc, out, stage, out_sem):
    slots = acc.shape[0]
    device = lax.axis_index("src") * n_rcv + lax.axis_index("rcv")

    def put(slot):
        return pltpu.make_async_copy(stage.at[slot], out.at[slot], out_sem.at[slot])

    def one(slot, carry):
        row_tile, col_tile, sign = slot_tiles(tiles, device * slots + slot)
        results = tile_product(
            [(weight[0], weight[1])],
            [jnp.stack([last[0, row_tile], last[1, row_tile]])],
            [(last[0, col_tile], last[1, col_tile])],
            sign,
        )
        for part in (0, 1):
            stage[slot, part] = acc[slot, part] + results[part]
        put(slot).start()
        return carry

    def drain(slot, carry):
        put(slot).wait()
        return carry

    lax.fori_loop(0, slots, one, 0, unroll=2 if slots % 2 == 0 else 1)
    lax.fori_loop(0, slots, drain, 0)


def solution(mesh):
    n_src, n_rcv = mesh.shape["src"], mesh.shape["rcv"]
    assert n_src % 2 == 0 and n_src > 2

    def body(panel, obliquity, panel_stations, tile_map, recorded):
        kd, width = panel.shape[1], panel.shape[2]
        slots, _, side, _ = recorded.shape
        held = width // side
        full = n_src // 2 - 1
        lines = pin(obliquity.reshape(2, -1, LANES).transpose(1, 0, 2), pltpu.HBM)
        tiles = pin(tile_map.T, pltpu.HBM)
        stations = pin(panel_stations, pltpu.HBM)
        hbm = pl.BlockSpec(memory_space=pltpu.HBM)
        vmem = pl.BlockSpec(memory_space=pltpu.VMEM)
        smem = pl.BlockSpec(memory_space=pltpu.SMEM)
        dma = pltpu.SemaphoreType.DMA
        block = (2, n_rcv * held, kd, side)
        acc, last, weight, mapped = pl.pallas_call(
            functools.partial(gather_kernel, n_src, n_rcv),
            out_shape=(
                pltpu.VMEM(recorded.shape, recorded.dtype),
                pltpu.VMEM(block, jnp.bfloat16),
                pltpu.VMEM((2, kd, LANES), jnp.float32),
                pltpu.SMEM(tiles.shape, tiles.dtype),
            ),
            in_specs=[hbm] * 5,
            out_specs=(vmem, vmem, vmem, smem),
            scratch_shapes=[pltpu.VMEM(block, jnp.bfloat16)] * (1 + 2 * full)
            + [
                pltpu.VMEM(panel.shape, jnp.float32),
                pltpu.VMEM(lines.shape, jnp.float32),
                pltpu.VMEM((2, panel_stations.shape[0], LANES), jnp.float32),
                pltpu.SMEM(panel_stations.shape, panel_stations.dtype),
                dma((2, full + 1, 2)),
                dma((2, full + 1, 2)),
                dma((2, full + 1, 2, n_rcv - 1)),
                dma((2, full + 1, 2, n_rcv - 1)),
                dma((2, 2, len(pieces(held)), n_rcv)),
                dma((2, 2, 2, len(pieces(held)))),
                dma((2, len(pieces(held)))),
                dma((4,)),
            ],
            compiler_params=pltpu.CompilerParams(
                collective_id=0, has_side_effects=True, vmem_limit_bytes=40 * 1024 * 1024
            ),
            name="ring_products",
        )(stations, tiles, pin(panel, pltpu.HBM), lines, pin(recorded, pltpu.HBM))
        return pl.pallas_call(
            functools.partial(finish_kernel, n_rcv),
            out_shape=jax.ShapeDtypeStruct(recorded.shape, recorded.dtype),
            in_specs=[smem, vmem, vmem, vmem],
            out_specs=hbm,
            scratch_shapes=[pltpu.VMEM(recorded.shape, recorded.dtype), dma((slots,))],
            compiler_params=pltpu.CompilerParams(vmem_limit_bytes=40 * 1024 * 1024),
            name="last_products",
        )(mapped, weight, last, acc)

    return jax.shard_map(
        body,
        mesh=mesh,
        in_specs=(
            P("freq", "src", "rcv"),
            P("freq", None),
            P(),
            P("freq", None),
            P(("src", "rcv"), "freq", None, None),
        ),
        out_specs=P(("src", "rcv"), "freq", None, None),
        check_vma=False,
    )
```

```python
import functools

import jax
import jax.numpy as jnp
from jax import lax
from jax.experimental import pallas as pl
from jax.experimental.pallas import tpu as pltpu
from jax.sharding import PartitionSpec as P

MESH = pl.DeviceIdType.MESH
pin = pltpu.with_memory_space_constraint
LANES = 128
ROWS = 8


def ring_position(index, n):
    if n % 2:
        return index
    half = index // 2
    odd = index % 2
    return odd * (n - 1 - half) + (1 - odd) * half


def ring_member(position, n):
    if n % 2:
        return position
    upper = position // (n // 2)
    return upper * (2 * (n - 1 - position) + 1) + (1 - upper) * 2 * position


def weighted_tile(weight, row_block, sign):
    spread = row_block.shape[-1] // LANES
    w_real = jnp.concatenate([weight[0] * sign] * spread, axis=1)
    w_imag = jnp.concatenate([weight[1] * sign] * spread, axis=1)
    p_real = row_block[0].astype(jnp.float32)
    p_imag = row_block[1].astype(jnp.float32)
    return [w_real * p_real - w_imag * p_imag, w_real * p_imag + w_imag * p_real]


def stack_rows(blocks):
    if blocks[0].shape[0] % 16:
        blocks = [b.astype(jnp.float32) for b in blocks]
    return jnp.concatenate(blocks, axis=0).astype(jnp.bfloat16)


def tile_product(weights, row_blocks, col_blocks, sign):
    lefts, reals, imags = [], [], []
    for weight, row_block, col_block in zip(weights, row_blocks, col_blocks):
        lefts += weighted_tile(weight, row_block, sign)
        reals += [col_block[0], -col_block[1]]
        imags += [col_block[1], col_block[0]]
    weighted = jnp.concatenate(lefts, axis=0).astype(jnp.bfloat16)
    form = (((0,), (0,)), ((), ()))
    return [
        lax.dot_general(weighted, stack_rows(c), form, preferred_element_type=jnp.float32)
        for c in (reals, imags)
    ]


def slot_tiles(tiles, at):
    row_tile, col_tile = tiles[0, at], tiles[1, at]
    sign = -(jnp.minimum(row_tile, 0) + 1).astype(jnp.float32)
    return jnp.maximum(row_tile, 0), jnp.maximum(col_tile, 0), sign


def pieces(held, small_first):
    small = min(2, held - 1) if small_first else 1
    if small_first:
        return [(0, small), (small, held - small)]
    half = (held - small) * 2 // 3
    return [(0, half), (half, held - small - half), (held - small, small)]


def gather_kernel(n_src, n_rcv, stations_in, tiles_in, panel, lines, recorded, acc, last, weight_out, tiles, *scratch):
    full = n_src // 2 - 1
    own = scratch[0]
    from_left = [own] + list(scratch[1 : 1 + full]) + [last]
    from_right = [own] + list(scratch[1 + full : 1 + 2 * full]) + [last]
    stage, obliquity, weight, stations, ring_send, ring_recv, pair_send, pair_recv, last_sems, first_sems, load_sem, local_sem = scratch[1 + 2 * full :]

    src = lax.axis_index("src")
    rcv = lax.axis_index("rcv")
    kd, side = own.shape[2], own.shape[3]
    slots = acc.shape[0]
    held = own.shape[1] // n_rcv
    cuts = pieces(held, True)
    ends = pieces(held, False)
    mine = pl.ds(rcv * held, held)
    pos = ring_position(src, n_src)
    right = ring_member((pos + 1) % n_src, n_src)
    left = ring_member((pos + n_src - 1) % n_src, n_src)

    def load(part, c):
        at = (part, slice(None), pl.ds(cuts[c][0] * side, cuts[c][1] * side))
        return pltpu.make_async_copy(panel.at[at], stage.at[at], load_sem.at[part, c])

    for part in (0, 1):
        load(part, 0).start()
    barrier = pltpu.get_barrier_semaphore()
    for peer in (left, right):
        pl.semaphore_signal(barrier, inc=1, device_id={"src": peer}, device_id_type=MESH)
    for off in range(1, n_rcv):
        pl.semaphore_signal(barrier, inc=1, device_id={"rcv": (rcv + off) % n_rcv}, device_id_type=MESH)

    for c in range(1, len(cuts)):
        for part in (0, 1):
            load(part, c).start()
    named = pltpu.make_async_copy(stations_in, stations, local_sem.at[2])
    mapped = pltpu.make_async_copy(tiles_in, tiles, local_sem.at[3])
    fetch = pltpu.make_async_copy(lines, obliquity, local_sem.at[0])
    fill = pltpu.make_async_copy(recorded, acc, local_sem.at[1])

    def convert(part, c):
        load(part, c).wait()
        for t in range(cuts[c][0], sum(cuts[c])):
            own[part, rcv * held + t] = stage[part, :, t * side : (t + 1) * side].astype(jnp.bfloat16)

    sides = ((0, from_left, right), (1, from_right, left))

    def ring_copy(d, step, part):
        _, blocks, peer = sides[d]
        return pltpu.make_async_remote_copy(
            src_ref=blocks[step].at[part, mine],
            dst_ref=blocks[step + 1].at[part, mine],
            send_sem=ring_send.at[d, step, part],
            recv_sem=ring_recv.at[d, step, part],
            device_id={"src": peer},
            device_id_type=MESH,
        )

    def pair_copy(d, step, part, off):
        block = sides[d][1][step].at[part, mine]
        return pltpu.make_async_remote_copy(
            src_ref=block,
            dst_ref=block,
            send_sem=pair_send.at[d, step, part, off - 1],
            recv_sem=pair_recv.at[d, step, part, off - 1],
            device_id={"rcv": (rcv + off) % n_rcv},
            device_id_type=MESH,
        )

    def first_ring(d, c):
        _, blocks, peer = sides[d]
        at = pl.ds(rcv * held + cuts[c][0], cuts[c][1])
        return pltpu.make_async_remote_copy(
            src_ref=own.at[d, at],
            dst_ref=blocks[1].at[d, at],
            send_sem=first_sems.at[0, d, c],
            recv_sem=first_sems.at[1, d, c],
            device_id={"src": peer},
            device_id_type=MESH,
        )

    def last_ring(d, c):
        _, blocks, peer = sides[d]
        at = pl.ds(rcv * held + ends[c][0], ends[c][1])
        return pltpu.make_async_remote_copy(
            src_ref=blocks[full].at[d, at],
            dst_ref=last.at[d, at],
            send_sem=last_sems.at[0, d, c, 0],
            recv_sem=last_sems.at[1, d, c, 0],
            device_id={"src": peer},
            device_id_type=MESH,
        )

    def last_pair(d, c, off):
        block = last.at[d, pl.ds(rcv * held + ends[c][0], ends[c][1])]
        return pltpu.make_async_remote_copy(
            src_ref=block,
            dst_ref=block,
            send_sem=last_sems.at[0, d, c, off],
            recv_sem=last_sems.at[1, d, c, off],
            device_id={"rcv": (rcv + off) % n_rcv},
            device_id_type=MESH,
        )

    def pairs(step, d):
        return d == 0 or step > 0

    def rows_of(owner):
        return pl.ds(pl.multiple_of(owner * kd, kd), kd)

    def product(blocks):
        def one(slot, carry):
            row_tile, col_tile, sign = slot_tiles(tiles, (src * n_rcv + rcv) * slots + slot)
            results = tile_product(
                [(weight[0, rows_of(owner), :], weight[1, rows_of(owner), :]) for _, owner in blocks],
                [jnp.stack([block[0, row_tile], block[1, row_tile]]) for block, _ in blocks],
                [(block[0, col_tile], block[1, col_tile]) for block, _ in blocks],
                sign,
            )
            for part in (0, 1):
                acc[slot, part] += results[part]
            return carry

        lax.fori_loop(0, slots, one, 0)

    def gather_weights():
        lane = lax.broadcasted_iota(jnp.int32, (ROWS, LANES), 1)
        row = lax.broadcasted_iota(jnp.int32, (ROWS, LANES), 0)

        def group(g, carry):
            real = jnp.zeros((ROWS, LANES), jnp.float32)
            imag = jnp.zeros((ROWS, LANES), jnp.float32)
            for u in range(ROWS):
                station = stations[g * ROWS + u]
                line = lax.div(station, LANES)
                pair = obliquity[line]
                hit = (row == u) & (lane == station - line * LANES)
                real = jnp.where(hit, pair[0:1], real)
                imag = jnp.where(hit, pair[1:2], imag)
            at = pl.ds(pl.multiple_of(g * ROWS, ROWS), ROWS)
            weight[0, at, :] = jnp.broadcast_to(jnp.sum(real, axis=1, keepdims=True), (ROWS, LANES))
            weight[1, at, :] = jnp.broadcast_to(jnp.sum(imag, axis=1, keepdims=True), (ROWS, LANES))
            return carry

        lax.fori_loop(0, weight.shape[1] // ROWS, group, 0)

    for c in range(len(cuts)):
        for part in (0, 1):
            convert(part, c)
            if part == 0 and c == 0:
                pl.semaphore_wait(barrier, 1 + n_rcv)
            first_ring(part, c).start()
    for d in (0, 1):
        ring_copy(d, 0, 1 - d).start()
    for part in (0, 1):
        for off in range(1, n_rcv):
            pair_copy(0, 0, part, off).start()
    for step in range(full + 1):
        for turn in (0, 1):
            for d in (0, 1):
                part = d if turn == 0 else 1 - d
                if step == 0:
                    continue
                if step == 1 and part == d:
                    for c in range(len(cuts)):
                        first_ring(d, c).wait_recv()
                else:
                    ring_copy(d, step - 1, part).wait_recv()
                if step < full:
                    ring_copy(d, step, part).start()
                elif part == d:
                    for c in range(len(ends)):
                        last_ring(d, c).start()
                for off in range(1, n_rcv):
                    pair_copy(d, step, part, off).start()
        if step == 0:
            fetch.start()
            named.start()
            mapped.start()
            fill.start()
            fetch.wait()
            named.wait()
            mapped.wait()
            gather_weights()
            fill.wait()
        for part in (0, 1):
            for d in (0, 1):
                if pairs(step, d):
                    for off in range(1, n_rcv):
                        pair_copy(d, step, part, off).wait_recv()
        before = ring_member((pos + n_src - step) % n_src, n_src)
        after = ring_member((pos + step) % n_src, n_src)
        if step == 0:
            blocks = [(own, src)]
        else:
            blocks = [(from_left[step], before), (from_right[step], after)]
        product(blocks)

    opposite = ring_member((pos + n_src // 2) % n_src, n_src)
    weight_out[...] = weight[:, rows_of(opposite), :]
    for step in range(full + 1):
        for part in (0, 1):
            for d in (0, 1):
                if step == 0 and part == d:
                    for c in range(len(cuts)):
                        first_ring(d, c).wait_send()
                elif step < full:
                    ring_copy(d, step, part).wait_send()
                if pairs(step, d):
                    for off in range(1, n_rcv):
                        pair_copy(d, step, part, off).wait_send()
    for c in range(len(ends)):
        for d in (0, 1):
            last_ring(d, c).wait_recv()
            for off in range(1, n_rcv):
                last_pair(d, c, off).start()
    for c in range(len(ends)):
        for d in (0, 1):
            for off in range(1, n_rcv):
                last_pair(d, c, off).wait_recv()
    for c in range(len(ends)):
        for d in (0, 1):
            last_ring(d, c).wait_send()
            for off in range(1, n_rcv):
                last_pair(d, c, off).wait_send()


def finish_kernel(n_rcv, tiles, weight, last, acc, out, stage, out_sem):
    slots = acc.shape[0]
    device = lax.axis_index("src") * n_rcv + lax.axis_index("rcv")

    def put(slot):
        return pltpu.make_async_copy(stage.at[slot], out.at[slot], out_sem.at[slot])

    def one(slot, carry):
        row_tile, col_tile, sign = slot_tiles(tiles, device * slots + slot)
        results = tile_product(
            [(weight[0], weight[1])],
            [jnp.stack([last[0, row_tile], last[1, row_tile]])],
            [(last[0, col_tile], last[1, col_tile])],
            sign,
        )
        for part in (0, 1):
            stage[slot, part] = acc[slot, part] + results[part]
        put(slot).start()
        return carry

    def drain(slot, carry):
        put(slot).wait()
        return carry

    lax.fori_loop(0, slots, one, 0, unroll=4 if slots % 4 == 0 else 1)
    lax.fori_loop(0, slots, drain, 0)


def solution(mesh):
    n_src, n_rcv = mesh.shape["src"], mesh.shape["rcv"]
    assert n_src % 2 == 0 and n_src > 2

    def body(panel, obliquity, panel_stations, tile_map, recorded):
        kd, width = panel.shape[1], panel.shape[2]
        slots, _, side, _ = recorded.shape
        held = width // side
        full = n_src // 2 - 1
        lines = pin(obliquity.reshape(2, -1, LANES).transpose(1, 0, 2), pltpu.HBM)
        tiles = pin(tile_map.T, pltpu.HBM)
        stations = pin(panel_stations, pltpu.HBM)
        hbm = pl.BlockSpec(memory_space=pltpu.HBM)
        vmem = pl.BlockSpec(memory_space=pltpu.VMEM)
        smem = pl.BlockSpec(memory_space=pltpu.SMEM)
        dma = pltpu.SemaphoreType.DMA
        block = (2, n_rcv * held, kd, side)
        acc, last, weight, mapped = pl.pallas_call(
            functools.partial(gather_kernel, n_src, n_rcv),
            out_shape=(
                pltpu.VMEM(recorded.shape, recorded.dtype),
                pltpu.VMEM(block, jnp.bfloat16),
                pltpu.VMEM((2, kd, LANES), jnp.float32),
                pltpu.SMEM(tiles.shape, tiles.dtype),
            ),
            in_specs=[hbm] * 5,
            out_specs=(vmem, vmem, vmem, smem),
            scratch_shapes=[pltpu.VMEM(block, jnp.bfloat16)] * (1 + 2 * full)
            + [
                pltpu.VMEM(panel.shape, jnp.float32),
                pltpu.VMEM(lines.shape, jnp.float32),
                pltpu.VMEM((2, panel_stations.shape[0], LANES), jnp.float32),
                pltpu.SMEM(panel_stations.shape, panel_stations.dtype),
                dma((2, full + 1, 2)),
                dma((2, full + 1, 2)),
                dma((2, full + 1, 2, n_rcv - 1)),
                dma((2, full + 1, 2, n_rcv - 1)),
                dma((2, 2, len(pieces(held, False)), n_rcv)),
                dma((2, 2, len(pieces(held, True)))),
                dma((2, len(pieces(held, True)))),
                dma((4,)),
            ],
            compiler_params=pltpu.CompilerParams(
                collective_id=0, has_side_effects=True, vmem_limit_bytes=40 * 1024 * 1024
            ),
            name="ring_products",
        )(stations, tiles, pin(panel, pltpu.HBM), lines, pin(recorded, pltpu.HBM))
        return pl.pallas_call(
            functools.partial(finish_kernel, n_rcv),
            out_shape=jax.ShapeDtypeStruct(recorded.shape, recorded.dtype),
            in_specs=[smem, vmem, vmem, vmem],
            out_specs=hbm,
            scratch_shapes=[pltpu.VMEM(recorded.shape, recorded.dtype), dma((slots,))],
            compiler_params=pltpu.CompilerParams(vmem_limit_bytes=40 * 1024 * 1024),
            name="last_products",
        )(mapped, weight, last, acc)

    return jax.shard_map(
        body,
        mesh=mesh,
        in_specs=(
            P("freq", "src", "rcv"),
            P("freq", None),
            P(),
            P("freq", None),
            P(("src", "rcv"), "freq", None, None),
        ),
        out_specs=P(("src", "rcv"), "freq", None, None),
        check_vma=False,
    )
```

```python
import functools

import jax
import jax.numpy as jnp
from jax import lax
from jax.experimental import pallas as pl
from jax.experimental.pallas import tpu as pltpu
from jax.sharding import PartitionSpec as P

MESH = pl.DeviceIdType.MESH
pin = pltpu.with_memory_space_constraint
LANES = 128
ROWS = 8


def ring_position(index, n):
    if n % 2:
        return index
    half = index // 2
    odd = index % 2
    return odd * (n - 1 - half) + (1 - odd) * half


def ring_member(position, n):
    if n % 2:
        return position
    upper = position // (n // 2)
    return upper * (2 * (n - 1 - position) + 1) + (1 - upper) * 2 * position


def weighted_tile(weight, row_block, sign):
    spread = row_block.shape[-1] // LANES
    w_real = jnp.concatenate([weight[0] * sign] * spread, axis=1)
    w_imag = jnp.concatenate([weight[1] * sign] * spread, axis=1)
    p_real = row_block[0].astype(jnp.float32)
    p_imag = row_block[1].astype(jnp.float32)
    return [w_real * p_real - w_imag * p_imag, w_real * p_imag + w_imag * p_real]


def stack_rows(blocks):
    if blocks[0].shape[0] % 16:
        blocks = [b.astype(jnp.float32) for b in blocks]
    return jnp.concatenate(blocks, axis=0).astype(jnp.bfloat16)


def tile_product(weights, row_blocks, col_blocks, sign):
    lefts, reals, imags = [], [], []
    for weight, row_block, col_block in zip(weights, row_blocks, col_blocks):
        lefts += weighted_tile(weight, row_block, sign)
        reals += [col_block[0], -col_block[1]]
        imags += [col_block[1], col_block[0]]
    weighted = jnp.concatenate(lefts, axis=0).astype(jnp.bfloat16)
    form = (((0,), (0,)), ((), ()))
    return [
        lax.dot_general(weighted, stack_rows(c), form, preferred_element_type=jnp.float32)
        for c in (reals, imags)
    ]


def slot_tiles(tiles, at):
    row_tile, col_tile = tiles[0, at], tiles[1, at]
    sign = -(jnp.minimum(row_tile, 0) + 1).astype(jnp.float32)
    return jnp.maximum(row_tile, 0), jnp.maximum(col_tile, 0), sign


def first_pieces(held):
    small = min(2, held - 1)
    return [(0, small), (small, held - small)]


def last_pieces(n_rcv, held):
    if n_rcv != 2 or held < 6:
        return [[(r * held, held - 1), (r * held + held - 1, 1)] for r in range(n_rcv)]
    return [[(0, held - 3), (held - 3, 2)], [(held + 1, held - 1), (held - 1, 2)]]


def gather_kernel(n_src, n_rcv, stations_in, tiles_in, panel, lines, recorded, acc, last, weight_out, tiles, *scratch):
    full = n_src // 2 - 1
    own = scratch[0]
    from_left = [own] + list(scratch[1 : 1 + full]) + [last]
    from_right = [own] + list(scratch[1 + full : 1 + 2 * full]) + [last]
    stage, obliquity, weight, stations, ring_send, ring_recv, pair_send, pair_recv, last_sems, spread_sems, first_sems, load_sem, local_sem = scratch[1 + 2 * full :]

    src = lax.axis_index("src")
    rcv = lax.axis_index("rcv")
    kd, side = own.shape[2], own.shape[3]
    slots = acc.shape[0]
    held = own.shape[1] // n_rcv
    cuts = first_pieces(held)
    plans = last_pieces(n_rcv, held)
    mine = pl.ds(rcv * held, held)
    pos = ring_position(src, n_src)
    right = ring_member((pos + 1) % n_src, n_src)
    left = ring_member((pos + n_src - 1) % n_src, n_src)

    def load(part, c):
        at = (part, slice(None), pl.ds(cuts[c][0] * side, cuts[c][1] * side))
        return pltpu.make_async_copy(panel.at[at], stage.at[at], load_sem.at[part, c])

    for part in (0, 1):
        load(part, 0).start()
    barrier = pltpu.get_barrier_semaphore()
    for peer in (left, right):
        pl.semaphore_signal(barrier, inc=1, device_id={"src": peer}, device_id_type=MESH)
    for off in range(1, n_rcv):
        pl.semaphore_signal(barrier, inc=1, device_id={"rcv": (rcv + off) % n_rcv}, device_id_type=MESH)

    for c in range(1, len(cuts)):
        for part in (0, 1):
            load(part, c).start()
    named = pltpu.make_async_copy(stations_in, stations, local_sem.at[2])
    mapped = pltpu.make_async_copy(tiles_in, tiles, local_sem.at[3])
    fetch = pltpu.make_async_copy(lines, obliquity, local_sem.at[0])
    fill = pltpu.make_async_copy(recorded, acc, local_sem.at[1])

    def convert(part, c):
        load(part, c).wait()
        for t in range(cuts[c][0], sum(cuts[c])):
            own[part, rcv * held + t] = stage[part, :, t * side : (t + 1) * side].astype(jnp.bfloat16)

    sides = ((0, from_left, right), (1, from_right, left))

    def ring_copy(d, step, part):
        _, blocks, peer = sides[d]
        return pltpu.make_async_remote_copy(
            src_ref=blocks[step].at[part, mine],
            dst_ref=blocks[step + 1].at[part, mine],
            send_sem=ring_send.at[d, step, part],
            recv_sem=ring_recv.at[d, step, part],
            device_id={"src": peer},
            device_id_type=MESH,
        )

    def pair_copy(d, step, part, off):
        block = sides[d][1][step].at[part, mine]
        return pltpu.make_async_remote_copy(
            src_ref=block,
            dst_ref=block,
            send_sem=pair_send.at[d, step, part, off - 1],
            recv_sem=pair_recv.at[d, step, part, off - 1],
            device_id={"rcv": (rcv + off) % n_rcv},
            device_id_type=MESH,
        )

    def first_ring(d, c):
        _, blocks, peer = sides[d]
        at = pl.ds(rcv * held + cuts[c][0], cuts[c][1])
        return pltpu.make_async_remote_copy(
            src_ref=own.at[d, at],
            dst_ref=blocks[1].at[d, at],
            send_sem=first_sems.at[0, d, c],
            recv_sem=first_sems.at[1, d, c],
            device_id={"src": peer},
            device_id_type=MESH,
        )

    def last_ring(core, d, c):
        _, blocks, peer = sides[d]
        at = (d, pl.ds(*plans[core][c]))
        return pltpu.make_async_remote_copy(
            src_ref=blocks[full].at[at],
            dst_ref=last.at[at],
            send_sem=last_sems.at[0, d, c],
            recv_sem=last_sems.at[1, d, c],
            device_id={"src": peer},
            device_id_type=MESH,
        )

    def last_pair(core, c, off):
        block = last.at[:, pl.ds(*plans[core][c])]
        return pltpu.make_async_remote_copy(
            src_ref=block,
            dst_ref=block,
            send_sem=spread_sems.at[0, c, off],
            recv_sem=spread_sems.at[1, c, off],
            device_id={"rcv": (rcv + off) % n_rcv},
            device_id_type=MESH,
        )

    def start_last(d, c):
        for core in range(n_rcv):
            pl.when(rcv == core)(lambda core=core: last_ring(core, d, c).start())

    def finish_last(core):
        others = [other for other in range(n_rcv) if other != core]
        for c in (0, 1):
            for d in (0, 1):
                last_ring(core, d, c).wait_recv()
            for off in range(1, n_rcv):
                last_pair(core, c, off).start()
        for c in (0, 1):
            for d in (0, 1):
                last_ring(core, d, c).wait_send()
        for c in (0, 1):
            for other in others:
                last_pair(other, c, (core - other) % n_rcv).wait_recv()
            for off in range(1, n_rcv):
                last_pair(core, c, off).wait_send()


    def pairs(step, d):
        return d == 0 or step > 0

    def rows_of(owner):
        return pl.ds(pl.multiple_of(owner * kd, kd), kd)

    def product(blocks):
        def one(slot, carry):
            row_tile, col_tile, sign = slot_tiles(tiles, (src * n_rcv + rcv) * slots + slot)
            results = tile_product(
                [(weight[0, rows_of(owner), :], weight[1, rows_of(owner), :]) for _, owner in blocks],
                [jnp.stack([block[0, row_tile], block[1, row_tile]]) for block, _ in blocks],
                [(block[0, col_tile], block[1, col_tile]) for block, _ in blocks],
                sign,
            )
            for part in (0, 1):
                acc[slot, part] += results[part]
            return carry

        lax.fori_loop(0, slots, one, 0)

    def gather_weights():
        lane = lax.broadcasted_iota(jnp.int32, (ROWS, LANES), 1)
        row = lax.broadcasted_iota(jnp.int32, (ROWS, LANES), 0)

        def group(g, carry):
            real = jnp.zeros((ROWS, LANES), jnp.float32)
            imag = jnp.zeros((ROWS, LANES), jnp.float32)
            for u in range(ROWS):
                station = stations[g * ROWS + u]
                line = lax.div(station, LANES)
                pair = obliquity[line]
                hit = (row == u) & (lane == station - line * LANES)
                real = jnp.where(hit, pair[0:1], real)
                imag = jnp.where(hit, pair[1:2], imag)
            at = pl.ds(pl.multiple_of(g * ROWS, ROWS), ROWS)
            weight[0, at, :] = jnp.broadcast_to(jnp.sum(real, axis=1, keepdims=True), (ROWS, LANES))
            weight[1, at, :] = jnp.broadcast_to(jnp.sum(imag, axis=1, keepdims=True), (ROWS, LANES))
            return carry

        lax.fori_loop(0, weight.shape[1] // ROWS, group, 0)

    for c in range(len(cuts)):
        for part in (0, 1):
            convert(part, c)
            if part == 0 and c == 0:
                pl.semaphore_wait(barrier, 1 + n_rcv)
            first_ring(part, c).start()
    for d in (0, 1):
        ring_copy(d, 0, 1 - d).start()
    for part in (0, 1):
        for off in range(1, n_rcv):
            pair_copy(0, 0, part, off).start()
    for step in range(full + 1):
        for turn in (0, 1):
            for d in (0, 1):
                part = d if turn == 0 else 1 - d
                if step == 0:
                    continue
                if step == 1 and part == d:
                    for c in range(len(cuts)):
                        first_ring(d, c).wait_recv()
                else:
                    ring_copy(d, step - 1, part).wait_recv()
                if step < full:
                    ring_copy(d, step, part).start()
                elif part == d:
                    start_last(d, 0)
                for off in range(1, n_rcv):
                    pair_copy(d, step, part, off).start()
        if step == 0:
            fetch.start()
            named.start()
            mapped.start()
            fill.start()
            fetch.wait()
            named.wait()
            mapped.wait()
            gather_weights()
            fill.wait()
        for part in (0, 1):
            for d in (0, 1):
                if pairs(step, d):
                    for off in range(1, n_rcv):
                        pair_copy(d, step, part, off).wait_recv()
        if step == full:
            for d in (0, 1):
                start_last(d, 1)
        before = ring_member((pos + n_src - step) % n_src, n_src)
        after = ring_member((pos + step) % n_src, n_src)
        if step == 0:
            blocks = [(own, src)]
        else:
            blocks = [(from_left[step], before), (from_right[step], after)]
        product(blocks)

    opposite = ring_member((pos + n_src // 2) % n_src, n_src)
    weight_out[...] = weight[:, rows_of(opposite), :]
    for step in range(full + 1):
        for part in (0, 1):
            for d in (0, 1):
                if step == 0 and part == d:
                    for c in range(len(cuts)):
                        first_ring(d, c).wait_send()
                elif step < full:
                    ring_copy(d, step, part).wait_send()
                if pairs(step, d):
                    for off in range(1, n_rcv):
                        pair_copy(d, step, part, off).wait_send()
    for core in range(n_rcv):
        pl.when(rcv == core)(functools.partial(finish_last, core))


def finish_kernel(n_rcv, tiles, weight, last, acc, out, stage, out_sem):
    slots = acc.shape[0]
    device = lax.axis_index("src") * n_rcv + lax.axis_index("rcv")

    def put(slot):
        return pltpu.make_async_copy(stage.at[slot], out.at[slot], out_sem.at[slot])

    def one(slot, carry):
        row_tile, col_tile, sign = slot_tiles(tiles, device * slots + slot)
        results = tile_product(
            [(weight[0], weight[1])],
            [jnp.stack([last[0, row_tile], last[1, row_tile]])],
            [(last[0, col_tile], last[1, col_tile])],
            sign,
        )
        for part in (0, 1):
            stage[slot, part] = acc[slot, part] + results[part]
        put(slot).start()
        return carry

    def drain(slot, carry):
        put(slot).wait()
        return carry

    lax.fori_loop(0, slots, one, 0, unroll=4 if slots % 4 == 0 else 1)
    lax.fori_loop(0, slots, drain, 0)


def solution(mesh):
    n_src, n_rcv = mesh.shape["src"], mesh.shape["rcv"]
    assert n_src % 2 == 0 and n_src > 2

    def body(panel, obliquity, panel_stations, tile_map, recorded):
        kd, width = panel.shape[1], panel.shape[2]
        slots, _, side, _ = recorded.shape
        held = width // side
        full = n_src // 2 - 1
        lines = pin(obliquity.reshape(2, -1, LANES).transpose(1, 0, 2), pltpu.HBM)
        tiles = pin(tile_map.T, pltpu.HBM)
        stations = pin(panel_stations, pltpu.HBM)
        hbm = pl.BlockSpec(memory_space=pltpu.HBM)
        vmem = pl.BlockSpec(memory_space=pltpu.VMEM)
        smem = pl.BlockSpec(memory_space=pltpu.SMEM)
        dma = pltpu.SemaphoreType.DMA
        block = (2, n_rcv * held, kd, side)
        acc, last, weight, mapped = pl.pallas_call(
            functools.partial(gather_kernel, n_src, n_rcv),
            out_shape=(
                pltpu.VMEM(recorded.shape, recorded.dtype),
                pltpu.VMEM(block, jnp.bfloat16),
                pltpu.VMEM((2, kd, LANES), jnp.float32),
                pltpu.SMEM(tiles.shape, tiles.dtype),
            ),
            in_specs=[hbm] * 5,
            out_specs=(vmem, vmem, vmem, smem),
            scratch_shapes=[pltpu.VMEM(block, jnp.bfloat16)] * (1 + 2 * full)
            + [
                pltpu.VMEM(panel.shape, jnp.float32),
                pltpu.VMEM(lines.shape, jnp.float32),
                pltpu.VMEM((2, panel_stations.shape[0], LANES), jnp.float32),
                pltpu.SMEM(panel_stations.shape, panel_stations.dtype),
                dma((2, full + 1, 2)),
                dma((2, full + 1, 2)),
                dma((2, full + 1, 2, n_rcv - 1)),
                dma((2, full + 1, 2, n_rcv - 1)),
                dma((2, 2, 2)),
                dma((2, 2, n_rcv)),
                dma((2, 2, len(first_pieces(held)))),
                dma((2, len(first_pieces(held)))),
                dma((4,)),
            ],
            compiler_params=pltpu.CompilerParams(
                collective_id=0, has_side_effects=True, vmem_limit_bytes=40 * 1024 * 1024
            ),
            name="ring_products",
        )(stations, tiles, pin(panel, pltpu.HBM), lines, pin(recorded, pltpu.HBM))
        return pl.pallas_call(
            functools.partial(finish_kernel, n_rcv),
            out_shape=jax.ShapeDtypeStruct(recorded.shape, recorded.dtype),
            in_specs=[smem, vmem, vmem, vmem],
            out_specs=hbm,
            scratch_shapes=[pltpu.VMEM(recorded.shape, recorded.dtype), dma((slots,))],
            compiler_params=pltpu.CompilerParams(vmem_limit_bytes=40 * 1024 * 1024),
            name="last_products",
        )(mapped, weight, last, acc)

    return jax.shard_map(
        body,
        mesh=mesh,
        in_specs=(
            P("freq", "src", "rcv"),
            P("freq", None),
            P(),
            P("freq", None),
            P(("src", "rcv"), "freq", None, None),
        ),
        out_specs=P(("src", "rcv"), "freq", None, None),
        check_vma=False,
    )
```

```python
import functools

import jax
import jax.numpy as jnp
from jax import lax
from jax.experimental import pallas as pl
from jax.experimental.pallas import tpu as pltpu
from jax.sharding import PartitionSpec as P

MESH = pl.DeviceIdType.MESH
pin = pltpu.with_memory_space_constraint
LANES = 128
ROWS = 8


def ring_position(index, n):
    if n % 2:
        return index
    half = index // 2
    odd = index % 2
    return odd * (n - 1 - half) + (1 - odd) * half


def ring_member(position, n):
    if n % 2:
        return position
    upper = position // (n // 2)
    return upper * (2 * (n - 1 - position) + 1) + (1 - upper) * 2 * position


def weighted_tile(weight, row_block, sign):
    spread = row_block.shape[-1] // LANES
    w_real = jnp.concatenate([weight[0] * sign] * spread, axis=1)
    w_imag = jnp.concatenate([weight[1] * sign] * spread, axis=1)
    p_real = row_block[0].astype(jnp.float32)
    p_imag = row_block[1].astype(jnp.float32)
    return [w_real * p_real - w_imag * p_imag, w_real * p_imag + w_imag * p_real]


def stack_rows(blocks):
    if blocks[0].shape[0] % 16:
        blocks = [b.astype(jnp.float32) for b in blocks]
    return jnp.concatenate(blocks, axis=0).astype(jnp.bfloat16)


def tile_product(weights, row_blocks, col_blocks, sign):
    lefts, reals, imags = [], [], []
    for weight, row_block, col_block in zip(weights, row_blocks, col_blocks):
        lefts += weighted_tile(weight, row_block, sign)
        reals += [col_block[0], -col_block[1]]
        imags += [col_block[1], col_block[0]]
    weighted = jnp.concatenate(lefts, axis=0).astype(jnp.bfloat16)
    form = (((0,), (0,)), ((), ()))
    return [
        lax.dot_general(weighted, stack_rows(c), form, preferred_element_type=jnp.float32)
        for c in (reals, imags)
    ]


def slot_tiles(tiles, at):
    row_tile, col_tile = tiles[0, at], tiles[1, at]
    sign = -(jnp.minimum(row_tile, 0) + 1).astype(jnp.float32)
    return jnp.maximum(row_tile, 0), jnp.maximum(col_tile, 0), sign


def first_pieces(held):
    small = min(4, held - 1)
    return [(0, small), (small, held - small)]


def last_pieces(n_rcv, held):
    if n_rcv != 2 or held < 6:
        return [[(r * held, held - 1), (r * held + held - 1, 1)] for r in range(n_rcv)]
    return [[(0, held - 3), (held - 3, 2)], [(held + 1, held - 1), (held - 1, 2)]]


def gather_kernel(n_src, n_rcv, stations_in, tiles_in, panel, lines, recorded, acc, last, weight_out, tiles, *scratch):
    full = n_src // 2 - 1
    own = scratch[0]
    from_left = [own] + list(scratch[1 : 1 + full]) + [last]
    from_right = [own] + list(scratch[1 + full : 1 + 2 * full]) + [last]
    stage, obliquity, weight, stations, ring_send, ring_recv, pair_send, pair_recv, last_sems, spread_sems, first_sems, load_sem, local_sem = scratch[1 + 2 * full :]

    src = lax.axis_index("src")
    rcv = lax.axis_index("rcv")
    kd, side = own.shape[2], own.shape[3]
    slots = acc.shape[0]
    held = own.shape[1] // n_rcv
    cuts = first_pieces(held)
    plans = last_pieces(n_rcv, held)
    mine = pl.ds(rcv * held, held)
    pos = ring_position(src, n_src)
    right = ring_member((pos + 1) % n_src, n_src)
    left = ring_member((pos + n_src - 1) % n_src, n_src)

    def load(part, c):
        at = (part, slice(None), pl.ds(cuts[c][0] * side, cuts[c][1] * side))
        return pltpu.make_async_copy(panel.at[at], stage.at[at], load_sem.at[part, c])

    barrier = pltpu.get_barrier_semaphore()
    for peer in (left, right):
        pl.semaphore_signal(barrier, inc=1, device_id={"src": peer}, device_id_type=MESH)
    for off in range(1, n_rcv):
        pl.semaphore_signal(barrier, inc=1, device_id={"rcv": (rcv + off) % n_rcv}, device_id_type=MESH)

    for c in range(len(cuts)):
        for part in (0, 1):
            load(part, c).start()
    named = pltpu.make_async_copy(stations_in, stations, local_sem.at[2])
    mapped = pltpu.make_async_copy(tiles_in, tiles, local_sem.at[3])
    fetch = pltpu.make_async_copy(lines, obliquity, local_sem.at[0])
    fill = pltpu.make_async_copy(recorded, acc, local_sem.at[1])

    def convert(part, c):
        load(part, c).wait()
        for t in range(cuts[c][0], sum(cuts[c])):
            own[part, rcv * held + t] = stage[part, :, t * side : (t + 1) * side].astype(jnp.bfloat16)

    sides = ((0, from_left, right), (1, from_right, left))

    def ring_copy(d, step, part):
        _, blocks, peer = sides[d]
        return pltpu.make_async_remote_copy(
            src_ref=blocks[step].at[part, mine],
            dst_ref=blocks[step + 1].at[part, mine],
            send_sem=ring_send.at[d, step, part],
            recv_sem=ring_recv.at[d, step, part],
            device_id={"src": peer},
            device_id_type=MESH,
        )

    def pair_copy(d, step, part, off):
        block = sides[d][1][step].at[part, mine]
        return pltpu.make_async_remote_copy(
            src_ref=block,
            dst_ref=block,
            send_sem=pair_send.at[d, step, part, off - 1],
            recv_sem=pair_recv.at[d, step, part, off - 1],
            device_id={"rcv": (rcv + off) % n_rcv},
            device_id_type=MESH,
        )

    def first_ring(d, c):
        _, blocks, peer = sides[d]
        at = pl.ds(rcv * held + cuts[c][0], cuts[c][1])
        return pltpu.make_async_remote_copy(
            src_ref=own.at[d, at],
            dst_ref=blocks[1].at[d, at],
            send_sem=first_sems.at[0, d, c],
            recv_sem=first_sems.at[1, d, c],
            device_id={"src": peer},
            device_id_type=MESH,
        )

    def last_ring(core, d, c):
        _, blocks, peer = sides[d]
        at = (d, pl.ds(*plans[core][c]))
        return pltpu.make_async_remote_copy(
            src_ref=blocks[full].at[at],
            dst_ref=last.at[at],
            send_sem=last_sems.at[0, d, c],
            recv_sem=last_sems.at[1, d, c],
            device_id={"src": peer},
            device_id_type=MESH,
        )

    def last_pair(core, c, off):
        block = last.at[:, pl.ds(*plans[core][c])]
        return pltpu.make_async_remote_copy(
            src_ref=block,
            dst_ref=block,
            send_sem=spread_sems.at[0, c, off],
            recv_sem=spread_sems.at[1, c, off],
            device_id={"rcv": (rcv + off) % n_rcv},
            device_id_type=MESH,
        )

    def start_last(d, c):
        for core in range(n_rcv):
            pl.when(rcv == core)(lambda core=core: last_ring(core, d, c).start())

    def finish_last(core):
        others = [other for other in range(n_rcv) if other != core]
        for c in (0, 1):
            for d in (0, 1):
                last_ring(core, d, c).wait_recv()
            for off in range(1, n_rcv):
                last_pair(core, c, off).start()
        for c in (0, 1):
            for d in (0, 1):
                last_ring(core, d, c).wait_send()
        for c in (0, 1):
            for other in others:
                last_pair(other, c, (core - other) % n_rcv).wait_recv()
            for off in range(1, n_rcv):
                last_pair(core, c, off).wait_send()


    def pairs(step, d):
        return d == 0 or step > 0

    def rows_of(owner):
        return pl.ds(pl.multiple_of(owner * kd, kd), kd)

    def product(blocks):
        def one(slot, carry):
            row_tile, col_tile, sign = slot_tiles(tiles, (src * n_rcv + rcv) * slots + slot)
            results = tile_product(
                [(weight[0, rows_of(owner), :], weight[1, rows_of(owner), :]) for _, owner in blocks],
                [jnp.stack([block[0, row_tile], block[1, row_tile]]) for block, _ in blocks],
                [(block[0, col_tile], block[1, col_tile]) for block, _ in blocks],
                sign,
            )
            for part in (0, 1):
                acc[slot, part] += results[part]
            return carry

        lax.fori_loop(0, slots, one, 0)

    def gather_weights():
        lane = lax.broadcasted_iota(jnp.int32, (ROWS, LANES), 1)
        row = lax.broadcasted_iota(jnp.int32, (ROWS, LANES), 0)

        def group(g, carry):
            real = jnp.zeros((ROWS, LANES), jnp.float32)
            imag = jnp.zeros((ROWS, LANES), jnp.float32)
            for u in range(ROWS):
                station = stations[g * ROWS + u]
                line = lax.div(station, LANES)
                pair = obliquity[line]
                hit = (row == u) & (lane == station - line * LANES)
                real = jnp.where(hit, pair[0:1], real)
                imag = jnp.where(hit, pair[1:2], imag)
            at = pl.ds(pl.multiple_of(g * ROWS, ROWS), ROWS)
            weight[0, at, :] = jnp.broadcast_to(jnp.sum(real, axis=1, keepdims=True), (ROWS, LANES))
            weight[1, at, :] = jnp.broadcast_to(jnp.sum(imag, axis=1, keepdims=True), (ROWS, LANES))
            return carry

        lax.fori_loop(0, weight.shape[1] // ROWS, group, 0)

    for c in range(len(cuts)):
        for part in (0, 1):
            convert(part, c)
            if part == 0 and c == 0:
                pl.semaphore_wait(barrier, 1 + n_rcv)
            first_ring(part, c).start()
    for d in (0, 1):
        ring_copy(d, 0, 1 - d).start()
    for part in (0, 1):
        for off in range(1, n_rcv):
            pair_copy(0, 0, part, off).start()
    for step in range(full + 1):
        for turn in (0, 1):
            for d in (0, 1):
                part = d if turn == 0 else 1 - d
                if step == 0:
                    continue
                if step == 1 and part == d:
                    for c in range(len(cuts)):
                        first_ring(d, c).wait_recv()
                else:
                    ring_copy(d, step - 1, part).wait_recv()
                if step < full:
                    ring_copy(d, step, part).start()
                elif part == d:
                    start_last(d, 0)
                for off in range(1, n_rcv):
                    pair_copy(d, step, part, off).start()
        if step == 0:
            fetch.start()
            named.start()
            mapped.start()
            fill.start()
            fetch.wait()
            named.wait()
            mapped.wait()
            gather_weights()
            fill.wait()
        for part in (0, 1):
            for d in (0, 1):
                if pairs(step, d):
                    for off in range(1, n_rcv):
                        pair_copy(d, step, part, off).wait_recv()
        if step == full:
            for d in (0, 1):
                start_last(d, 1)
        before = ring_member((pos + n_src - step) % n_src, n_src)
        after = ring_member((pos + step) % n_src, n_src)
        if step == 0:
            blocks = [(own, src)]
        else:
            blocks = [(from_left[step], before), (from_right[step], after)]
        product(blocks)

    opposite = ring_member((pos + n_src // 2) % n_src, n_src)
    weight_out[...] = weight[:, rows_of(opposite), :]
    for step in range(full + 1):
        for part in (0, 1):
            for d in (0, 1):
                if step == 0 and part == d:
                    for c in range(len(cuts)):
                        first_ring(d, c).wait_send()
                elif step < full:
                    ring_copy(d, step, part).wait_send()
                if pairs(step, d):
                    for off in range(1, n_rcv):
                        pair_copy(d, step, part, off).wait_send()
    for core in range(n_rcv):
        pl.when(rcv == core)(functools.partial(finish_last, core))


def finish_kernel(n_rcv, tiles, weight, last, acc, out, stage, out_sem):
    slots = acc.shape[0]
    device = lax.axis_index("src") * n_rcv + lax.axis_index("rcv")

    def put(slot):
        return pltpu.make_async_copy(stage.at[slot], out.at[slot], out_sem.at[slot])

    def one(slot, carry):
        row_tile, col_tile, sign = slot_tiles(tiles, device * slots + slot)
        results = tile_product(
            [(weight[0], weight[1])],
            [jnp.stack([last[0, row_tile], last[1, row_tile]])],
            [(last[0, col_tile], last[1, col_tile])],
            sign,
        )
        for part in (0, 1):
            stage[slot, part] = acc[slot, part] + results[part]
        put(slot).start()
        return carry

    def drain(slot, carry):
        put(slot).wait()
        return carry

    lax.fori_loop(0, slots, one, 0, unroll=4 if slots % 4 == 0 else 1)
    lax.fori_loop(0, slots, drain, 0)


def solution(mesh):
    n_src, n_rcv = mesh.shape["src"], mesh.shape["rcv"]
    assert n_src % 2 == 0 and n_src > 2

    def body(panel, obliquity, panel_stations, tile_map, recorded):
        kd, width = panel.shape[1], panel.shape[2]
        slots, _, side, _ = recorded.shape
        held = width // side
        full = n_src // 2 - 1
        lines = pin(obliquity.reshape(2, -1, LANES).transpose(1, 0, 2), pltpu.HBM)
        tiles = pin(tile_map.T, pltpu.HBM)
        stations = pin(panel_stations, pltpu.HBM)
        hbm = pl.BlockSpec(memory_space=pltpu.HBM)
        vmem = pl.BlockSpec(memory_space=pltpu.VMEM)
        smem = pl.BlockSpec(memory_space=pltpu.SMEM)
        dma = pltpu.SemaphoreType.DMA
        block = (2, n_rcv * held, kd, side)
        acc, last, weight, mapped = pl.pallas_call(
            functools.partial(gather_kernel, n_src, n_rcv),
            out_shape=(
                pltpu.VMEM(recorded.shape, recorded.dtype),
                pltpu.VMEM(block, jnp.bfloat16),
                pltpu.VMEM((2, kd, LANES), jnp.float32),
                pltpu.SMEM(tiles.shape, tiles.dtype),
            ),
            in_specs=[hbm] * 5,
            out_specs=(vmem, vmem, vmem, smem),
            scratch_shapes=[pltpu.VMEM(block, jnp.bfloat16)] * (1 + 2 * full)
            + [
                pltpu.VMEM(panel.shape, jnp.float32),
                pltpu.VMEM(lines.shape, jnp.float32),
                pltpu.VMEM((2, panel_stations.shape[0], LANES), jnp.float32),
                pltpu.SMEM(panel_stations.shape, panel_stations.dtype),
                dma((2, full + 1, 2)),
                dma((2, full + 1, 2)),
                dma((2, full + 1, 2, n_rcv - 1)),
                dma((2, full + 1, 2, n_rcv - 1)),
                dma((2, 2, 2)),
                dma((2, 2, n_rcv)),
                dma((2, 2, len(first_pieces(held)))),
                dma((2, len(first_pieces(held)))),
                dma((4,)),
            ],
            compiler_params=pltpu.CompilerParams(
                collective_id=0, has_side_effects=True, vmem_limit_bytes=40 * 1024 * 1024
            ),
            name="ring_products",
        )(stations, tiles, pin(panel, pltpu.HBM), lines, pin(recorded, pltpu.HBM))
        return pl.pallas_call(
            functools.partial(finish_kernel, n_rcv),
            out_shape=jax.ShapeDtypeStruct(recorded.shape, recorded.dtype),
            in_specs=[smem, vmem, vmem, vmem],
            out_specs=hbm,
            scratch_shapes=[pltpu.VMEM(recorded.shape, recorded.dtype), dma((slots,))],
            compiler_params=pltpu.CompilerParams(vmem_limit_bytes=40 * 1024 * 1024),
            name="last_products",
        )(mapped, weight, last, acc)

    return jax.shard_map(
        body,
        mesh=mesh,
        in_specs=(
            P("freq", "src", "rcv"),
            P("freq", None),
            P(),
            P("freq", None),
            P(("src", "rcv"), "freq", None, None),
        ),
        out_specs=P(("src", "rcv"), "freq", None, None),
        check_vma=False,
    )
```

```python
import functools

import jax
import jax.numpy as jnp
from jax import lax
from jax.experimental import pallas as pl
from jax.experimental.pallas import tpu as pltpu
from jax.sharding import PartitionSpec as P

MESH = pl.DeviceIdType.MESH
pin = pltpu.with_memory_space_constraint
LANES = 128
ROWS = 8


def ring_position(index, n):
    if n % 2:
        return index
    half = index // 2
    odd = index % 2
    return odd * (n - 1 - half) + (1 - odd) * half


def ring_member(position, n):
    if n % 2:
        return position
    upper = position // (n // 2)
    return upper * (2 * (n - 1 - position) + 1) + (1 - upper) * 2 * position


def weighted_tile(weight, row_block, sign):
    spread = row_block.shape[-1] // LANES
    w_real = jnp.concatenate([weight[0] * sign] * spread, axis=1)
    w_imag = jnp.concatenate([weight[1] * sign] * spread, axis=1)
    p_real = row_block[0].astype(jnp.float32)
    p_imag = row_block[1].astype(jnp.float32)
    return [w_real * p_real - w_imag * p_imag, w_real * p_imag + w_imag * p_real]


def stack_rows(blocks):
    if blocks[0].shape[0] % 16:
        blocks = [b.astype(jnp.float32) for b in blocks]
    return jnp.concatenate(blocks, axis=0).astype(jnp.bfloat16)


def tile_product(weights, row_blocks, col_blocks, sign):
    lefts, reals, imags = [], [], []
    for weight, row_block, col_block in zip(weights, row_blocks, col_blocks):
        lefts += weighted_tile(weight, row_block, sign)
        reals += [col_block[0], -col_block[1]]
        imags += [col_block[1], col_block[0]]
    weighted = jnp.concatenate(lefts, axis=0).astype(jnp.bfloat16)
    form = (((0,), (0,)), ((), ()))
    return [
        lax.dot_general(weighted, stack_rows(c), form, preferred_element_type=jnp.float32)
        for c in (reals, imags)
    ]


def slot_tiles(tiles, at):
    row_tile, col_tile = tiles[0, at], tiles[1, at]
    sign = -(jnp.minimum(row_tile, 0) + 1).astype(jnp.float32)
    return jnp.maximum(row_tile, 0), jnp.maximum(col_tile, 0), sign


def first_pieces(held):
    small = min(2, held - 1)
    return [(0, small), (small, held - small)]


def last_pieces(n_rcv, held):
    if n_rcv != 2 or held < 6:
        return [[(r * held, held - 1), (r * held + held - 1, 1)] for r in range(n_rcv)]
    return [[(0, held - 5), (held - 5, 3)], [(held + 2, held - 2), (held - 2, 4)]]


def gather_kernel(n_src, n_rcv, stations_in, tiles_in, panel, lines, recorded, acc, last, weight_out, tiles, *scratch):
    full = n_src // 2 - 1
    own = scratch[0]
    from_left = [own] + list(scratch[1 : 1 + full]) + [last]
    from_right = [own] + list(scratch[1 + full : 1 + 2 * full]) + [last]
    stage, obliquity, weight, stations, ring_send, ring_recv, pair_send, pair_recv, last_sems, spread_sems, first_sems, load_sem, local_sem = scratch[1 + 2 * full :]

    src = lax.axis_index("src")
    rcv = lax.axis_index("rcv")
    kd, side = own.shape[2], own.shape[3]
    slots = acc.shape[0]
    held = own.shape[1] // n_rcv
    cuts = first_pieces(held)
    plans = last_pieces(n_rcv, held)
    mine = pl.ds(rcv * held, held)
    pos = ring_position(src, n_src)
    right = ring_member((pos + 1) % n_src, n_src)
    left = ring_member((pos + n_src - 1) % n_src, n_src)

    def load(part, c):
        at = (part, slice(None), pl.ds(cuts[c][0] * side, cuts[c][1] * side))
        return pltpu.make_async_copy(panel.at[at], stage.at[at], load_sem.at[part, c])

    for part in (0, 1):
        load(part, 0).start()
    barrier = pltpu.get_barrier_semaphore()
    for peer in (left, right):
        pl.semaphore_signal(barrier, inc=1, device_id={"src": peer}, device_id_type=MESH)
    for off in range(1, n_rcv):
        pl.semaphore_signal(barrier, inc=1, device_id={"rcv": (rcv + off) % n_rcv}, device_id_type=MESH)

    for c in range(1, len(cuts)):
        for part in (0, 1):
            load(part, c).start()
    named = pltpu.make_async_copy(stations_in, stations, local_sem.at[2])
    mapped = pltpu.make_async_copy(tiles_in, tiles, local_sem.at[3])
    fetch = pltpu.make_async_copy(lines, obliquity, local_sem.at[0])
    fill = pltpu.make_async_copy(recorded, acc, local_sem.at[1])

    def convert(part, c):
        load(part, c).wait()
        for t in range(cuts[c][0], sum(cuts[c])):
            own[part, rcv * held + t] = stage[part, :, t * side : (t + 1) * side].astype(jnp.bfloat16)

    sides = ((0, from_left, right), (1, from_right, left))

    def ring_copy(d, step, part):
        _, blocks, peer = sides[d]
        return pltpu.make_async_remote_copy(
            src_ref=blocks[step].at[part, mine],
            dst_ref=blocks[step + 1].at[part, mine],
            send_sem=ring_send.at[d, step, part],
            recv_sem=ring_recv.at[d, step, part],
            device_id={"src": peer},
            device_id_type=MESH,
        )

    def pair_copy(d, step, part, off):
        block = sides[d][1][step].at[part, mine]
        return pltpu.make_async_remote_copy(
            src_ref=block,
            dst_ref=block,
            send_sem=pair_send.at[d, step, part, off - 1],
            recv_sem=pair_recv.at[d, step, part, off - 1],
            device_id={"rcv": (rcv + off) % n_rcv},
            device_id_type=MESH,
        )

    def first_ring(d, c):
        _, blocks, peer = sides[d]
        at = pl.ds(rcv * held + cuts[c][0], cuts[c][1])
        return pltpu.make_async_remote_copy(
            src_ref=own.at[d, at],
            dst_ref=blocks[1].at[d, at],
            send_sem=first_sems.at[0, d, c],
            recv_sem=first_sems.at[1, d, c],
            device_id={"src": peer},
            device_id_type=MESH,
        )

    def last_ring(core, d, c):
        _, blocks, peer = sides[d]
        at = (d, pl.ds(*plans[core][c]))
        return pltpu.make_async_remote_copy(
            src_ref=blocks[full].at[at],
            dst_ref=last.at[at],
            send_sem=last_sems.at[0, d, c],
            recv_sem=last_sems.at[1, d, c],
            device_id={"src": peer},
            device_id_type=MESH,
        )

    def last_pair(core, c, off):
        block = last.at[:, pl.ds(*plans[core][c])]
        return pltpu.make_async_remote_copy(
            src_ref=block,
            dst_ref=block,
            send_sem=spread_sems.at[0, c, off],
            recv_sem=spread_sems.at[1, c, off],
            device_id={"rcv": (rcv + off) % n_rcv},
            device_id_type=MESH,
        )

    def start_last(d, c):
        for core in range(n_rcv):
            pl.when(rcv == core)(lambda core=core: last_ring(core, d, c).start())

    def finish_last(core):
        others = [other for other in range(n_rcv) if other != core]
        for c in (0, 1):
            for d in (0, 1):
                last_ring(core, d, c).wait_recv()
            for off in range(1, n_rcv):
                last_pair(core, c, off).start()
        for c in (0, 1):
            for d in (0, 1):
                last_ring(core, d, c).wait_send()
        for c in (0, 1):
            for other in others:
                last_pair(other, c, (core - other) % n_rcv).wait_recv()
            for off in range(1, n_rcv):
                last_pair(core, c, off).wait_send()


    def pairs(step, d):
        return d == 0 or step > 0

    def rows_of(owner):
        return pl.ds(pl.multiple_of(owner * kd, kd), kd)

    def product(blocks):
        def one(slot, carry):
            row_tile, col_tile, sign = slot_tiles(tiles, (src * n_rcv + rcv) * slots + slot)
            results = tile_product(
                [(weight[0, rows_of(owner), :], weight[1, rows_of(owner), :]) for _, owner in blocks],
                [jnp.stack([block[0, row_tile], block[1, row_tile]]) for block, _ in blocks],
                [(block[0, col_tile], block[1, col_tile]) for block, _ in blocks],
                sign,
            )
            for part in (0, 1):
                acc[slot, part] += results[part]
            return carry

        lax.fori_loop(0, slots, one, 0)

    def gather_weights():
        lane = lax.broadcasted_iota(jnp.int32, (ROWS, LANES), 1)
        row = lax.broadcasted_iota(jnp.int32, (ROWS, LANES), 0)

        def group(g, carry):
            real = jnp.zeros((ROWS, LANES), jnp.float32)
            imag = jnp.zeros((ROWS, LANES), jnp.float32)
            for u in range(ROWS):
                station = stations[g * ROWS + u]
                line = lax.div(station, LANES)
                pair = obliquity[line]
                hit = (row == u) & (lane == station - line * LANES)
                real = jnp.where(hit, pair[0:1], real)
                imag = jnp.where(hit, pair[1:2], imag)
            at = pl.ds(pl.multiple_of(g * ROWS, ROWS), ROWS)
            weight[0, at, :] = jnp.broadcast_to(jnp.sum(real, axis=1, keepdims=True), (ROWS, LANES))
            weight[1, at, :] = jnp.broadcast_to(jnp.sum(imag, axis=1, keepdims=True), (ROWS, LANES))
            return carry

        lax.fori_loop(0, weight.shape[1] // ROWS, group, 0)

    for c in range(len(cuts)):
        for part in (0, 1):
            convert(part, c)
            if part == 0 and c == 0:
                pl.semaphore_wait(barrier, 1 + n_rcv)
            first_ring(part, c).start()
    for d in (0, 1):
        ring_copy(d, 0, 1 - d).start()
    for part in (0, 1):
        for off in range(1, n_rcv):
            pair_copy(0, 0, part, off).start()
    for step in range(full + 1):
        for turn in (0, 1):
            for d in (0, 1):
                part = d if turn == 0 else 1 - d
                if step == 0:
                    continue
                if step == 1 and part == d:
                    for c in range(len(cuts)):
                        first_ring(d, c).wait_recv()
                else:
                    ring_copy(d, step - 1, part).wait_recv()
                if step < full:
                    ring_copy(d, step, part).start()
                elif part == d:
                    start_last(d, 0)
                for off in range(1, n_rcv):
                    pair_copy(d, step, part, off).start()
        if step == 0:
            fetch.start()
            named.start()
            mapped.start()
            fill.start()
            fetch.wait()
            named.wait()
            mapped.wait()
            gather_weights()
            fill.wait()
        for part in (0, 1):
            for d in (0, 1):
                if pairs(step, d):
                    for off in range(1, n_rcv):
                        pair_copy(d, step, part, off).wait_recv()
        if step == full:
            for d in (0, 1):
                start_last(d, 1)
        before = ring_member((pos + n_src - step) % n_src, n_src)
        after = ring_member((pos + step) % n_src, n_src)
        if step == 0:
            blocks = [(own, src)]
        else:
            blocks = [(from_left[step], before), (from_right[step], after)]
        product(blocks)

    opposite = ring_member((pos + n_src // 2) % n_src, n_src)
    weight_out[...] = weight[:, rows_of(opposite), :]
    for step in range(full + 1):
        for part in (0, 1):
            for d in (0, 1):
                if step == 0 and part == d:
                    for c in range(len(cuts)):
                        first_ring(d, c).wait_send()
                elif step < full:
                    ring_copy(d, step, part).wait_send()
                if pairs(step, d):
                    for off in range(1, n_rcv):
                        pair_copy(d, step, part, off).wait_send()
    for core in range(n_rcv):
        pl.when(rcv == core)(functools.partial(finish_last, core))


def finish_kernel(n_rcv, tiles, weight, last, acc, out, stage, out_sem):
    slots = acc.shape[0]
    device = lax.axis_index("src") * n_rcv + lax.axis_index("rcv")

    def put(slot):
        return pltpu.make_async_copy(stage.at[slot], out.at[slot], out_sem.at[slot])

    def one(slot, carry):
        row_tile, col_tile, sign = slot_tiles(tiles, device * slots + slot)
        results = tile_product(
            [(weight[0], weight[1])],
            [jnp.stack([last[0, row_tile], last[1, row_tile]])],
            [(last[0, col_tile], last[1, col_tile])],
            sign,
        )
        for part in (0, 1):
            stage[slot, part] = acc[slot, part] + results[part]
        put(slot).start()
        return carry

    def drain(slot, carry):
        put(slot).wait()
        return carry

    lax.fori_loop(0, slots, one, 0, unroll=4 if slots % 4 == 0 else 1)
    lax.fori_loop(0, slots, drain, 0)


def solution(mesh):
    n_src, n_rcv = mesh.shape["src"], mesh.shape["rcv"]
    assert n_src % 2 == 0 and n_src > 2

    def body(panel, obliquity, panel_stations, tile_map, recorded):
        kd, width = panel.shape[1], panel.shape[2]
        slots, _, side, _ = recorded.shape
        held = width // side
        full = n_src // 2 - 1
        lines = pin(obliquity.reshape(2, -1, LANES).transpose(1, 0, 2), pltpu.HBM)
        tiles = pin(tile_map.T, pltpu.HBM)
        stations = pin(panel_stations, pltpu.HBM)
        hbm = pl.BlockSpec(memory_space=pltpu.HBM)
        vmem = pl.BlockSpec(memory_space=pltpu.VMEM)
        smem = pl.BlockSpec(memory_space=pltpu.SMEM)
        dma = pltpu.SemaphoreType.DMA
        block = (2, n_rcv * held, kd, side)
        acc, last, weight, mapped = pl.pallas_call(
            functools.partial(gather_kernel, n_src, n_rcv),
            out_shape=(
                pltpu.VMEM(recorded.shape, recorded.dtype),
                pltpu.VMEM(block, jnp.bfloat16),
                pltpu.VMEM((2, kd, LANES), jnp.float32),
                pltpu.SMEM(tiles.shape, tiles.dtype),
            ),
            in_specs=[hbm] * 5,
            out_specs=(vmem, vmem, vmem, smem),
            scratch_shapes=[pltpu.VMEM(block, jnp.bfloat16)] * (1 + 2 * full)
            + [
                pltpu.VMEM(panel.shape, jnp.float32),
                pltpu.VMEM(lines.shape, jnp.float32),
                pltpu.VMEM((2, panel_stations.shape[0], LANES), jnp.float32),
                pltpu.SMEM(panel_stations.shape, panel_stations.dtype),
                dma((2, full + 1, 2)),
                dma((2, full + 1, 2)),
                dma((2, full + 1, 2, n_rcv - 1)),
                dma((2, full + 1, 2, n_rcv - 1)),
                dma((2, 2, 2)),
                dma((2, 2, n_rcv)),
                dma((2, 2, len(first_pieces(held)))),
                dma((2, len(first_pieces(held)))),
                dma((4,)),
            ],
            compiler_params=pltpu.CompilerParams(
                collective_id=0, has_side_effects=True, vmem_limit_bytes=40 * 1024 * 1024
            ),
            name="ring_products",
        )(stations, tiles, pin(panel, pltpu.HBM), lines, pin(recorded, pltpu.HBM))
        return pl.pallas_call(
            functools.partial(finish_kernel, n_rcv),
            out_shape=jax.ShapeDtypeStruct(recorded.shape, recorded.dtype),
            in_specs=[smem, vmem, vmem, vmem],
            out_specs=hbm,
            scratch_shapes=[pltpu.VMEM(recorded.shape, recorded.dtype), dma((slots,))],
            compiler_params=pltpu.CompilerParams(vmem_limit_bytes=40 * 1024 * 1024),
            name="last_products",
        )(mapped, weight, last, acc)

    return jax.shard_map(
        body,
        mesh=mesh,
        in_specs=(
            P("freq", "src", "rcv"),
            P("freq", None),
            P(),
            P("freq", None),
            P(("src", "rcv"), "freq", None, None),
        ),
        out_specs=P(("src", "rcv"), "freq", None, None),
        check_vma=False,
    )
```
